32 devices in a mesh: gx: 4 (over z), gy: 4 (over y, core), af: 2 (over x).
Axes of the slice: x: 2, y: 2, z: 4, core: 2. Of those that a mesh axis runs over, the one named last changes fastest.
Arguments:
- points: bfloat16 [1024, 256], P(('gx', 'gy'), 'af'), may hold values from -12 to 12
- targets: float32 [1024, 16], P(('gx', 'gy')), may hold values from -6 to 6
Outputs:
- solution: float32 [1024, 16], P(('gx', 'gy'))
- residual: float32 [1024, 16], P(('gx', 'gy'))
The draws below stay inside these ranges and needn't reach their ends.
All inputs are finite; a program needn't handle non-finite values.
Results may differ from the reference program's by a relative error of at most 0.025.
Values may be sent and summed in bfloat16 or wider, within the bound.
No kernel may reach another device: no remote copies, remote signals or barrier semaphores. Data moves between devices by JAX's collectives and lax.ppermute only.
A program may use at most 64 MiB of HBM per device.

```python
import jax
import jax.numpy as jnp
from jax import lax

F = 256
R = 16
P_DEV = 64
ITERS = 2
N_PTS = 1024


def draw_points(key, part):
    keys = jax.random.split(jax.random.fold_in(key, 11), 5)
    labels = jax.random.randint(keys[0], (N_PTS,), 0, 16)
    one_hot = (labels[:, None] == jnp.arange(16, dtype=jnp.int32)[None, :]).astype(jnp.float32)
    centres = 1.4 * jax.random.normal(keys[1], (16, F), jnp.float32)
    spread = jnp.exp(jax.random.uniform(keys[3], (16,), jnp.float32, 0.0, 0.47))
    noise = jax.random.normal(keys[4], (N_PTS, F), jnp.float32)
    row_centres = jnp.dot(one_hot, centres, precision=lax.Precision.HIGHEST)
    row_spread = jnp.dot(one_hot, spread, precision=lax.Precision.HIGHEST)
    values = row_centres + row_spread[:, None] * noise
    return jnp.clip(values, -12.0, 12.0).astype(jnp.bfloat16)


def block_scale(own_key, extent, pieces, smallest, high):
    factor_of, own = 1.0, jax.random.fold_in(own_key, 6)
    for dim, shards_of in pieces:
        draws = jnp.exp(jax.random.uniform(jax.random.fold_in(own, dim), (shards_of,), jnp.float32, smallest / len(pieces), high / len(pieces)))
        factor_of = factor_of * jnp.repeat(draws, extent[dim] // shards_of).reshape([-1 if axis == dim else 1 for axis in range(len(extent))])
    return factor_of


def bell_draw(own_key, dims, scale, bound, pieces=(), kind=jnp.bfloat16):
    drawn = jax.random.normal(own_key, dims, jnp.float32) * scale
    if len(pieces) > 0:
        drawn = block_scale(own_key, dims, pieces, -0.22, 0.18) * drawn
    return jnp.clip(drawn, min=-bound, max=bound).astype(kind)


def setup_inputs(seed: int = 0) -> dict:
    streams_of = jax.random.split(jax.random.key(seed), 3)
    points = draw_points(jax.random.fold_in(streams_of[2], 71), 0)
    targets = bell_draw(streams_of[1], (N_PTS, R), 1.0, 6.0, ((0, 16),), jnp.float32)
    return dict(points=points, targets=targets)


def operate(coords, norms, vector):
    lowered = lax.optimization_barrier(vector.astype(jnp.bfloat16)).astype(jnp.float32)
    scale = 0.5 / F
    blocks = coords.reshape(N_PTS // P_DEV, P_DEV, F)
    block_norms = norms.reshape(N_PTS // P_DEV, P_DEV)

    def one_block(pair):
        rows, row_norms = pair
        inner = jnp.dot(rows, coords.T)
        distance = row_norms[:, None] + norms[None, :] - 2.0 * inner
        kernel = lax.optimization_barrier(jnp.exp(-scale * distance).astype(jnp.bfloat16)).astype(jnp.float32)
        return jnp.dot(kernel, lowered)

    product = lax.map(one_block, (blocks, block_norms)).reshape(N_PTS, R)
    return product + 0.1 * vector


def reference(points, targets):
    coords = points.astype(jnp.float32)
    norms = jnp.sum(coords * coords, axis=1)
    solution = jnp.zeros_like(targets)
    residual = targets
    direction = targets
    norm_now = jnp.sum(residual * residual, axis=0)
    for step in range(ITERS):
        image = operate(coords, norms, direction)
        alpha = norm_now / jnp.sum(direction * image, axis=0)
        solution = solution + alpha * direction
        residual = residual - alpha * image
        norm_next = jnp.sum(residual * residual, axis=0)
        direction = residual + (norm_next / norm_now) * direction
        norm_now = norm_next
    return solution, residual
```

```python
import functools
import math

import jax
import jax.numpy as jnp
from jax import lax
from jax.experimental import pallas as pl
from jax.experimental.pallas import tpu as pltpu
from jax.sharding import PartitionSpec as P

ITERS = 2


def point_norms(block):
    wide_block = block.astype(jnp.float32)
    return jnp.sum(wide_block * wide_block, axis=1)


def kernel_times(row_slab, slab_norms, col_slab, col_slab_norms, col_vector, scale):
    inner = lax.dot_general(
        row_slab, col_slab, (((1,), (1,)), ((), ())), preferred_element_type=jnp.float32
    )
    distance = slab_norms[:, None] + col_slab_norms[None, :] - 2.0 * inner
    kernel = jnp.exp(-scale * distance).astype(jnp.bfloat16)
    return jnp.dot(kernel, col_vector, preferred_element_type=jnp.float32)


def split_size(count):
    block_size = count
    while block_size > 1024 and block_size % 2 == 0:
        block_size = block_size // 2
    return block_size


def split_local(points, targets):
    whole_feat = lax.all_gather(points, "af", axis=1, tiled=True)
    norms = point_norms(whole_feat)
    half_rows = whole_feat.shape[0] // 2
    start_row = lax.axis_index("af") * half_rows
    my_points = lax.dynamic_slice_in_dim(whole_feat, start_row, half_rows, 0)
    scale = 0.5 / whole_feat.shape[1]
    stored_points = lax.all_gather(my_points, ("gx", "gy"), axis=0, tiled=True)
    stored_norms = point_norms(stored_points)

    def operate(vector):
        lowered = vector.astype(jnp.bfloat16)
        my_vector = lax.dynamic_slice_in_dim(lowered, start_row, half_rows, 0)
        empty = jnp.zeros(vector.shape, jnp.float32)
        piece = lax.all_gather(my_vector, ("gx", "gy"), axis=0, tiled=True)
        count = piece.shape[0]
        block_size = split_size(count)

        def one_block(carry, index):
            offset = index * block_size
            col_slab = lax.dynamic_slice_in_dim(stored_points, offset, block_size, 0)
            col_slab_norms = lax.dynamic_slice_in_dim(stored_norms, offset, block_size, 0)
            vector_slab = lax.dynamic_slice_in_dim(piece, offset, block_size, 0)
            return (
                carry
                + kernel_times(whole_feat, norms, col_slab, col_slab_norms, vector_slab, scale),
                None,
            )

        result, unused = lax.scan(
            one_block, empty, jnp.arange(count // block_size, dtype=jnp.int32)
        )
        return lax.psum(result, "af") + 0.1 * vector

    def two_products(values, image):
        return lax.psum(
            (jnp.sum(values * values, axis=0), jnp.sum(values * image, axis=0)), ("gx", "gy")
        )

    solution = jnp.zeros_like(targets)
    residual = targets
    image = operate(residual)
    norm_now, product = two_products(residual, image)
    alpha = norm_now / product
    direction = residual
    along = image
    for step in range(ITERS):
        solution = solution + alpha * direction
        residual = residual - alpha * along
        if step + 1 < ITERS:
            image = operate(residual)
            norm_next, product = two_products(residual, image)
            ratio = norm_next / norm_now
            alpha = norm_next / (product - ratio * norm_next / alpha)
            direction = residual + ratio * direction
            along = image + ratio * along
            norm_now = norm_next
    return (solution, residual)


AXES = ("gx", "gy", "af")
LANES = 128
KERNEL_BYTES = 8 * 1024 * 1024


def exact_parts(wide):
    high = wide.astype(jnp.bfloat16)
    low = (wide - high.astype(jnp.float32)).astype(jnp.bfloat16)
    return high, low


def row_dot(a, b):
    return lax.dot_general(a, b, (((1,), (1,)), ((), ())), preferred_element_type=jnp.float32)


def solve_kernel(blocks, rows, *refs):
    targets_ref, solution_ref, residual_ref, coords, kernel = refs[-5:]
    pairs = [(refs[k], refs[k + 1]) for k in range(0, len(refs) - 5, 2)]
    group = blocks * rows
    half = pairs[0][1].shape[1]
    columns = targets_ref.shape[0]
    packed = []
    for index, (main, other) in enumerate(pairs):
        coords[index * group : (index + 1) * group, :half] = main[:group, :]
        coords[index * group : (index + 1) * group, half:] = other[...]
        for block in range(blocks):
            both = main[group + block * columns : group + (block + 1) * columns, :].astype(
                jnp.float32
            )
            packed.append(both[:, :rows] + both[:, rows:])
    packed[0] = targets_ref[...]
    targets = jnp.concatenate(packed, axis=1)
    lowered = targets.astype(jnp.bfloat16)

    every = coords[...]
    features = every.shape[1]
    count = every.shape[0]
    turn = math.log2(math.e) * 0.5 / features
    wide = every.astype(jnp.float32)
    high, low = exact_parts(wide * wide)
    ones = jnp.ones((8, features), jnp.bfloat16)
    along = -turn * (row_dot(ones, high) + row_dot(ones, low))[:1, :]
    panel = 2 * LANES
    image = jnp.zeros((columns, count), jnp.float32)
    for start in range(0, count, panel):
        mine = coords[start : start + panel, :]
        inner = row_dot(mine, every)
        wide = mine.astype(jnp.float32)
        down = -turn * jnp.sum(wide * wide, axis=1, keepdims=True)
        part = jnp.exp2((2.0 * turn) * inner + down + along).astype(jnp.bfloat16)
        kernel[start : start + panel, :] = part
        image = image + jnp.dot(
            lowered[:, start : start + panel], part, preferred_element_type=jnp.float32
        )

    def total(a, b):
        return jnp.sum(a * b, axis=1, keepdims=True)

    solution = jnp.zeros_like(targets)
    residual = targets
    direction = targets
    norm_now = total(residual, residual)
    for step in range(ITERS):
        if step > 0:
            image = jnp.dot(
                direction.astype(jnp.bfloat16), kernel[...], preferred_element_type=jnp.float32
            )
        image = image + 0.1 * direction
        alpha = norm_now / total(direction, image)
        solution = solution + alpha * direction
        residual = residual - alpha * image
        if step + 1 < ITERS:
            norm_next = total(residual, residual)
            direction = residual + (norm_next / norm_now) * direction
            norm_now = norm_next
    solution_ref[...] = solution[:, :rows]
    residual_ref[...] = residual[:, :rows]


def swap(array, sizes, flips):
    pairs = []
    for place in range(math.prod(sizes)):
        rest, far, weight = place, 0, 1
        for size, flip in zip(reversed(sizes), reversed(flips)):
            far += ((rest % size) ^ flip) * weight
            rest, weight = rest // size, weight * size
        pairs.append((place, far))
    return lax.ppermute(array, AXES, pairs)


def whole_local(sizes, points, targets):
    across, along, features = sizes
    rows = points.shape[0]
    turned = targets.T
    high, low = exact_parts(turned)
    packed = jnp.concatenate([high, low], axis=1)
    own = jnp.concatenate([points, packed], axis=0)
    far = [swap(own, sizes, (k, 0, 0)) for k in reversed(range(1, across))]
    far = [own] + far[::-1]
    coords = jnp.concatenate([block[:rows] for block in far], axis=0)
    main = jnp.concatenate([coords] + [block[rows:] for block in far], axis=0)
    moves = [(y, x) for y in range(0, along, 2) for x in range(features)]
    got = {}
    for y, x in reversed(moves):
        if (y, x) == (0, 0):
            got[y, x] = main
        else:
            got[y, x] = swap(coords if x else main, sizes, (0, y, x))
    ordered = [got[move] for move in moves]
    ordered = ordered + [swap(block, sizes, (0, 1, 0)) for block in ordered]
    count = rows * across * along
    width = points.shape[1] * features
    out = jax.ShapeDtypeStruct(turned.shape, jnp.float32)
    vmem = pl.BlockSpec(memory_space=pltpu.VMEM)
    solution, residual = pl.pallas_call(
        functools.partial(solve_kernel, across, rows),
        out_shape=(out, out),
        in_specs=[vmem] * (len(ordered) + 1),
        out_specs=(vmem, vmem),
        scratch_shapes=[
            pltpu.VMEM((count, width), jnp.bfloat16),
            pltpu.VMEM((count, count), jnp.bfloat16),
        ],
        cost_estimate=pl.CostEstimate(
            flops=2 * count * count * (width + LANES),
            transcendentals=count * count,
            bytes_accessed=2 * count * width,
        ),
    )(*ordered, turned)
    return solution.T, residual.T


def fits_whole(sizes, points, targets):
    across, along, features = sizes
    rows, width = points.shape
    count = rows * across * along
    powers = all(size & (size - 1) == 0 for size in sizes)
    return (
        powers
        and along > 1
        and features == 2
        and 2 * rows == LANES
        and width == LANES
        and targets.shape[1] == 16
        and 2 * count * count <= KERNEL_BYTES
    )


def local(sizes, points, targets):
    if fits_whole(sizes, points, targets):
        return whole_local(sizes, points, targets)
    return split_local(points, targets)


def solution(mesh):
    placed = (P(("gx", "gy"), "af"), P(("gx", "gy"), None))
    sizes = tuple(mesh.shape[axis] for axis in AXES)
    return jax.shard_map(
        functools.partial(local, sizes),
        mesh=mesh,
        in_specs=placed,
        out_specs=(P(("gx", "gy"), None), P(("gx", "gy"), None)),
        check_vma=False,
    )
```

```python
import functools
import math

import jax
import jax.numpy as jnp
from jax import lax
from jax.experimental import pallas as pl
from jax.experimental.pallas import tpu as pltpu
from jax.sharding import PartitionSpec as P

ITERS = 2


def point_norms(block):
    wide_block = block.astype(jnp.float32)
    return jnp.sum(wide_block * wide_block, axis=1)


def kernel_times(row_slab, slab_norms, col_slab, col_slab_norms, col_vector, scale):
    inner = lax.dot_general(
        row_slab, col_slab, (((1,), (1,)), ((), ())), preferred_element_type=jnp.float32
    )
    distance = slab_norms[:, None] + col_slab_norms[None, :] - 2.0 * inner
    kernel = jnp.exp(-scale * distance).astype(jnp.bfloat16)
    return jnp.dot(kernel, col_vector, preferred_element_type=jnp.float32)


def split_size(count):
    block_size = count
    while block_size > 1024 and block_size % 2 == 0:
        block_size = block_size // 2
    return block_size


def split_local(points, targets):
    whole_feat = lax.all_gather(points, "af", axis=1, tiled=True)
    norms = point_norms(whole_feat)
    half_rows = whole_feat.shape[0] // 2
    start_row = lax.axis_index("af") * half_rows
    my_points = lax.dynamic_slice_in_dim(whole_feat, start_row, half_rows, 0)
    scale = 0.5 / whole_feat.shape[1]
    stored_points = lax.all_gather(my_points, ("gx", "gy"), axis=0, tiled=True)
    stored_norms = point_norms(stored_points)

    def operate(vector):
        lowered = vector.astype(jnp.bfloat16)
        my_vector = lax.dynamic_slice_in_dim(lowered, start_row, half_rows, 0)
        empty = jnp.zeros(vector.shape, jnp.float32)
        piece = lax.all_gather(my_vector, ("gx", "gy"), axis=0, tiled=True)
        count = piece.shape[0]
        block_size = split_size(count)

        def one_block(carry, index):
            offset = index * block_size
            col_slab = lax.dynamic_slice_in_dim(stored_points, offset, block_size, 0)
            col_slab_norms = lax.dynamic_slice_in_dim(stored_norms, offset, block_size, 0)
            vector_slab = lax.dynamic_slice_in_dim(piece, offset, block_size, 0)
            return (
                carry
                + kernel_times(whole_feat, norms, col_slab, col_slab_norms, vector_slab, scale),
                None,
            )

        result, unused = lax.scan(
            one_block, empty, jnp.arange(count // block_size, dtype=jnp.int32)
        )
        return lax.psum(result, "af") + 0.1 * vector

    def two_products(values, image):
        return lax.psum(
            (jnp.sum(values * values, axis=0), jnp.sum(values * image, axis=0)), ("gx", "gy")
        )

    solution = jnp.zeros_like(targets)
    residual = targets
    image = operate(residual)
    norm_now, product = two_products(residual, image)
    alpha = norm_now / product
    direction = residual
    along = image
    for step in range(ITERS):
        solution = solution + alpha * direction
        residual = residual - alpha * along
        if step + 1 < ITERS:
            image = operate(residual)
            norm_next, product = two_products(residual, image)
            ratio = norm_next / norm_now
            alpha = norm_next / (product - ratio * norm_next / alpha)
            direction = residual + ratio * direction
            along = image + ratio * along
            norm_now = norm_next
    return (solution, residual)


AXES = ("gx", "gy", "af")
LANES = 128
KERNEL_BYTES = 8 * 1024 * 1024


def exact_parts(wide):
    high = wide.astype(jnp.bfloat16)
    low = (wide - high.astype(jnp.float32)).astype(jnp.bfloat16)
    return high, low


def row_dot(a, b):
    return lax.dot_general(a, b, (((1,), (1,)), ((), ())), preferred_element_type=jnp.float32)


def solve_kernel(blocks, rows, *refs):
    targets_ref, solution_ref, residual_ref, coords, kernel = refs[-5:]
    pairs = [(refs[k], refs[k + 1]) for k in range(0, len(refs) - 5, 2)]
    group = blocks * rows
    half = pairs[0][1].shape[1]
    columns = targets_ref.shape[0]
    packed = []
    for index, (main, other) in enumerate(pairs):
        coords[index * group : (index + 1) * group, :half] = main[:group, :]
        coords[index * group : (index + 1) * group, half:] = other[...]
        for block in range(blocks):
            both = main[group + block * columns : group + (block + 1) * columns, :].astype(
                jnp.float32
            )
            packed.append(both[:, :rows] + both[:, rows:])
    packed[0] = targets_ref[...]
    targets = jnp.concatenate(packed, axis=1)
    lowered = targets.astype(jnp.bfloat16)

    every = coords[...]
    features = every.shape[1]
    count = every.shape[0]
    turn = math.log2(math.e) * 0.5 / features
    wide = every.astype(jnp.float32)
    high, low = exact_parts(wide * wide)
    ones = jnp.ones((8, features), jnp.bfloat16)
    along = -turn * (row_dot(ones, high) + row_dot(ones, low))[:1, :]
    panel = 2 * LANES
    image = jnp.zeros((columns, count), jnp.float32)
    for start in range(0, count, panel):
        mine = coords[start : start + panel, :]
        inner = row_dot(mine, every)
        wide = mine.astype(jnp.float32)
        down = -turn * jnp.sum(wide * wide, axis=1, keepdims=True)
        part = jnp.exp2((2.0 * turn) * inner + down + along).astype(jnp.bfloat16)
        kernel[start : start + panel, :] = part
        image = image + jnp.dot(
            lowered[:, start : start + panel], part, preferred_element_type=jnp.float32
        )

    def total(a, b):
        return jnp.sum(a * b, axis=1, keepdims=True)

    solution = jnp.zeros_like(targets)
    residual = targets
    direction = targets
    norm_now = total(residual, residual)
    for step in range(ITERS):
        if step > 0:
            image = jnp.dot(
                direction.astype(jnp.bfloat16), kernel[...], preferred_element_type=jnp.float32
            )
        image = image + 0.1 * direction
        alpha = norm_now / total(direction, image)
        solution = solution + alpha * direction
        residual = residual - alpha * image
        if step + 1 < ITERS:
            norm_next = total(residual, residual)
            direction = residual + (norm_next / norm_now) * direction
            norm_now = norm_next
    solution_ref[...] = solution[:, :rows]
    residual_ref[...] = residual[:, :rows]


def swap(array, sizes, flips):
    pairs = []
    for place in range(math.prod(sizes)):
        rest, far, weight = place, 0, 1
        for size, flip in zip(reversed(sizes), reversed(flips)):
            far += ((rest % size) ^ flip) * weight
            rest, weight = rest // size, weight * size
        pairs.append((place, far))
    return lax.ppermute(array, AXES, pairs)


def whole_local(sizes, points, targets):
    across, along, features = sizes
    rows = points.shape[0]
    turned = targets.T
    high, low = exact_parts(turned)
    packed = jnp.concatenate([high, low], axis=1)
    own = jnp.concatenate([points, packed], axis=0)
    far = [swap(own, sizes, (k, 0, 0)) for k in reversed(range(1, across))]
    far = [own] + far[::-1]
    coords = jnp.concatenate([block[:rows] for block in far], axis=0)
    main = jnp.concatenate([coords] + [block[rows:] for block in far], axis=0)
    moves = [(y, x) for y in range(0, along, 2) for x in range(features)]
    got = {}
    for y, x in reversed(moves):
        if (y, x) == (0, 0):
            got[y, x] = main
        else:
            got[y, x] = swap(coords if x else main, sizes, (0, y, x))
    ordered = [got[move] for move in moves]
    ordered = ordered + [swap(block, sizes, (0, 1, 0)) for block in ordered]
    count = rows * across * along
    width = points.shape[1] * features
    out = jax.ShapeDtypeStruct(turned.shape, jnp.float32)
    vmem = pl.BlockSpec(memory_space=pltpu.VMEM)
    solution, residual = pl.pallas_call(
        functools.partial(solve_kernel, across, rows),
        out_shape=(out, out),
        in_specs=[vmem] * (len(ordered) + 1),
        out_specs=(vmem, vmem),
        scratch_shapes=[
            pltpu.VMEM((count, width), jnp.bfloat16),
            pltpu.VMEM((count, count), jnp.bfloat16),
        ],
        cost_estimate=pl.CostEstimate(
            flops=2 * count * count * (width + LANES),
            transcendentals=count * count,
            bytes_accessed=2 * count * width,
        ),
    )(*[pltpu.with_memory_space_constraint(array, pltpu.VMEM) for array in (*ordered, turned)])
    return solution.T, residual.T


def fits_whole(sizes, points, targets):
    across, along, features = sizes
    rows, width = points.shape
    count = rows * across * along
    powers = all(size & (size - 1) == 0 for size in sizes)
    return (
        powers
        and along > 1
        and features == 2
        and 2 * rows == LANES
        and width == LANES
        and targets.shape[1] == 16
        and 2 * count * count <= KERNEL_BYTES
    )


def local(sizes, points, targets):
    if fits_whole(sizes, points, targets):
        return whole_local(sizes, points, targets)
    return split_local(points, targets)


def solution(mesh):
    placed = (P(("gx", "gy"), "af"), P(("gx", "gy"), None))
    sizes = tuple(mesh.shape[axis] for axis in AXES)
    return jax.shard_map(
        functools.partial(local, sizes),
        mesh=mesh,
        in_specs=placed,
        out_specs=(P(("gx", "gy"), None), P(("gx", "gy"), None)),
        check_vma=False,
    )
```

```python
import functools
import math

import jax
import jax.numpy as jnp
from jax import lax
from jax.experimental import pallas as pl
from jax.experimental.pallas import tpu as pltpu
from jax.sharding import PartitionSpec as P


ITERS = 2


def point_norms(block):
    wide_block = block.astype(jnp.float32)
    return jnp.sum(wide_block * wide_block, axis=1)


def kernel_times(row_slab, slab_norms, col_slab, col_slab_norms, col_vector, scale):
    inner = lax.dot_general(
        row_slab, col_slab, (((1,), (1,)), ((), ())), preferred_element_type=jnp.float32
    )
    distance = slab_norms[:, None] + col_slab_norms[None, :] - 2.0 * inner
    kernel = jnp.exp(-scale * distance).astype(jnp.bfloat16)
    return jnp.dot(kernel, col_vector, preferred_element_type=jnp.float32)


def split_size(count):
    block_size = count
    while block_size > 1024 and block_size % 2 == 0:
        block_size = block_size // 2
    return block_size


def split_local(points, targets):
    whole_feat = lax.all_gather(points, "af", axis=1, tiled=True)
    norms = point_norms(whole_feat)
    half_rows = whole_feat.shape[0] // 2
    start_row = lax.axis_index("af") * half_rows
    my_points = lax.dynamic_slice_in_dim(whole_feat, start_row, half_rows, 0)
    scale = 0.5 / whole_feat.shape[1]
    stored_points = lax.all_gather(my_points, ("gx", "gy"), axis=0, tiled=True)
    stored_norms = point_norms(stored_points)

    def operate(vector):
        lowered = vector.astype(jnp.bfloat16)
        my_vector = lax.dynamic_slice_in_dim(lowered, start_row, half_rows, 0)
        empty = jnp.zeros(vector.shape, jnp.float32)
        piece = lax.all_gather(my_vector, ("gx", "gy"), axis=0, tiled=True)
        count = piece.shape[0]
        block_size = split_size(count)

        def one_block(carry, index):
            offset = index * block_size
            col_slab = lax.dynamic_slice_in_dim(stored_points, offset, block_size, 0)
            col_slab_norms = lax.dynamic_slice_in_dim(stored_norms, offset, block_size, 0)
            vector_slab = lax.dynamic_slice_in_dim(piece, offset, block_size, 0)
            return (
                carry
                + kernel_times(whole_feat, norms, col_slab, col_slab_norms, vector_slab, scale),
                None,
            )

        result, _ = lax.scan(one_block, empty, jnp.arange(count // block_size, dtype=jnp.int32))
        return lax.psum(result, "af") + 0.1 * vector

    def two_products(values, image):
        return lax.psum(
            (jnp.sum(values * values, axis=0), jnp.sum(values * image, axis=0)), ("gx", "gy")
        )

    solution = jnp.zeros_like(targets)
    residual = targets
    image = operate(residual)
    norm_now, product = two_products(residual, image)
    alpha = norm_now / product
    direction = residual
    along = image
    for step in range(ITERS):
        solution = solution + alpha * direction
        residual = residual - alpha * along
        if step + 1 < ITERS:
            image = operate(residual)
            norm_next, product = two_products(residual, image)
            ratio = norm_next / norm_now
            alpha = norm_next / (product - ratio * norm_next / alpha)
            direction = residual + ratio * direction
            along = image + ratio * along
            norm_now = norm_next
    return (solution, residual)


AXES = ("gx", "gy", "af")
LANES = 128
PANEL = 4 * LANES
KERNEL_BYTES = 8 * 1024 * 1024


def exact_parts(wide):
    high = lax.reduce_precision(wide, exponent_bits=8, mantissa_bits=7)
    return high.astype(jnp.bfloat16), (wide - high).astype(jnp.bfloat16)


def row_dot(a, b):
    return lax.dot_general(a, b, (((1,), (1,)), ((), ())), preferred_element_type=jnp.float32)


def plain_dot(a, b):
    return jnp.dot(a, b, preferred_element_type=jnp.float32)


def turn_of(features):
    return math.log2(math.e) * 0.5 / features


def unpack(blocks, rows, columns, groups, coords, parts):
    group = blocks * rows
    packed = []
    for index, (main, other) in enumerate(groups):
        width = main.shape[1]
        coords[index * group : (index + 1) * group, :width] = main[:group, :]
        coords[index * group : (index + 1) * group, width:] = other[...]
        for block in range(blocks):
            both = main[group + block * columns : group + (block + 1) * columns, :]
            packed.append(both.astype(jnp.float32))
    left = lax.broadcasted_iota(jnp.int32, packed[0].shape, 1) < rows
    for k in range(len(packed) // 2):
        one, two = packed[2 * k : 2 * k + 2]
        high = jnp.where(left, one, pltpu.roll(two, rows, 1))
        low = jnp.where(left, pltpu.roll(one, rows, 1), two)
        stacked = jnp.concatenate([high, low], axis=0).astype(jnp.bfloat16)
        parts[:, k * LANES : (k + 1) * LANES] = stacked


def scaled_norms(coords, start, down, along):
    turn = turn_of(coords.shape[1])
    wide = coords[start : start + PANEL, :].astype(jnp.float32)
    column = -turn * jnp.sum(wide * wide, axis=1, keepdims=True)
    spread = jnp.broadcast_to(column, (PANEL, LANES))
    down[start : start + PANEL, :] = spread
    shape = (LANES, LANES)
    eye = lax.broadcasted_iota(jnp.int32, shape, 0) == lax.broadcasted_iota(jnp.int32, shape, 1)
    for k in range(PANEL // LANES):
        picked = jnp.where(eye, spread[k * LANES : (k + 1) * LANES, :], 0.0)
        row = jnp.sum(picked, axis=0, keepdims=True)
        first = start + k * LANES
        along[:, first : first + LANES] = jnp.broadcast_to(row, (8, LANES))


def kernel_columns(coords, down, along, kernel, begin, end, start):
    turn = turn_of(coords.shape[1])
    inner = row_dot(coords[begin:end, :], coords[start : start + PANEL, :])
    column = down[begin:end, :]
    column = jnp.concatenate([column] * (PANEL // LANES), axis=1)
    power = (2.0 * turn) * inner + column + along[:1, start : start + PANEL]
    kernel[begin:end, start : start + PANEL] = jnp.exp2(power).astype(jnp.bfloat16)


def join(parts):
    half = parts.shape[0] // 2
    return parts[:half, :] + parts[half:, :]


def own_kernel(blocks, rows, count, *refs):
    coords, down, along, kernel, parts, image = refs[count:]
    groups = [(refs[k], refs[k + 1]) for k in range(0, count, 2)]
    unpack(blocks, rows, parts.shape[0] // 2, groups, coords, parts)
    half = coords.shape[0]
    for i in range(0, half, PANEL):
        scaled_norms(coords, i, down, along)
    for j in range(0, half, PANEL):
        kernel_columns(coords, down, along, kernel, 0, half, j)
        image[:, j : j + PANEL] = plain_dot(parts[...], kernel[:, j : j + PANEL])


def solve_kernel(blocks, rows, count, *refs):
    own, own_down, own_along, own_block, own_parts, own_image = refs[count : count + 6]
    solution_ref, residual_ref = refs[count + 6 : count + 8]
    coords, down, along, kernel, parts = refs[count + 8 :]
    groups = [(refs[k], refs[k + 1]) for k in range(0, count, 2)]
    half = own.shape[0]
    whole = 2 * half
    unpack(
        blocks, rows, parts.shape[0] // 2, groups, coords.at[half:, :], parts.at[:, half:]
    )
    coords[:half, :] = own[...]
    down[:half, :] = own_down[...]
    along[:, :half] = own_along[...]
    parts[:, :half] = own_parts[...]
    kernel[:half, :half] = own_block[...]
    for i in range(half, whole, PANEL):
        scaled_norms(coords, i, down, along)
    for j in range(half, whole, PANEL):
        kernel_columns(coords, down, along, kernel, 0, whole, j)
    for j in range(0, half, PANEL):
        kernel_columns(coords, down, along, kernel, half, whole, j)
    products = [
        own_image[...] + plain_dot(parts[:, half:], kernel[half:, :half]),
        plain_dot(parts[...], kernel[:, half:]),
    ]
    targets = join(parts[...].astype(jnp.float32))

    def total_of(a, b):
        return jnp.sum(a * b, axis=1, keepdims=True)

    image = join(jnp.concatenate(products, axis=1)) + 0.1 * targets
    high = image.astype(jnp.bfloat16)
    low = (image - high.astype(jnp.float32)).astype(jnp.bfloat16)
    stacked = jnp.concatenate([high, low], axis=0)
    again = join(plain_dot(stacked, kernel[...])) + 0.1 * image
    norm_first = total_of(targets, targets)
    alpha = norm_first / total_of(targets, image)
    residual = targets - alpha * image
    norm_next = total_of(residual, residual)
    ratio = norm_next / norm_first
    direction = residual + ratio * targets
    along_direction = (1.0 + ratio) * image - alpha * again
    step = norm_next / total_of(direction, along_direction)
    solution_ref[...] = (alpha * targets + step * direction)[:, :rows]
    residual_ref[...] = (residual - step * along_direction)[:, :rows]


def swap(array, sizes, flips):
    pairs = []
    for place in range(math.prod(sizes)):
        rest, far, weight = place, 0, 1
        for size, flip in zip(reversed(sizes), reversed(flips)):
            far += ((rest % size) ^ flip) * weight
            rest, weight = rest // size, weight * size
        pairs.append((place, far))
    return lax.ppermute(array, AXES, pairs)


def in_vmem(arrays):
    return [pltpu.with_memory_space_constraint(array, pltpu.VMEM) for array in arrays]


def whole_local(sizes, points, targets):
    across, along, features = sizes
    rows = points.shape[0]
    columns = targets.shape[1]
    high, low = exact_parts(targets.T)
    packed = jnp.concatenate([high, low], axis=1)
    own = jnp.concatenate([points, packed], axis=0)
    far = [swap(own, sizes, (k, 0, 0)) for k in reversed(range(1, across))]
    far = [own] + far[::-1]
    coords = jnp.concatenate([block[:rows] for block in far], axis=0)
    main = jnp.concatenate([coords] + [block[rows:] for block in far], axis=0)
    moves = [(y, x) for y in range(0, along, 2) for x in range(features)]
    got = {}
    for y, x in reversed(moves):
        if (y, x) == (0, 0):
            got[y, x] = main
        else:
            got[y, x] = swap(coords if x else main, sizes, (0, y, x))
    ours = [got[move] for move in moves]
    theirs = [swap(block, sizes, (0, 1, 0)) for block in ours]
    half = rows * across * along // 2
    width = points.shape[1] * features
    f32, bf16 = jnp.float32, jnp.bfloat16
    vmem = pl.BlockSpec(memory_space=pltpu.VMEM)
    kept = (
        pltpu.VMEM((half, width), bf16),
        pltpu.VMEM((half, LANES), f32),
        pltpu.VMEM((8, half), f32),
        pltpu.VMEM((half, half), bf16),
        pltpu.VMEM((2 * columns, half), bf16),
        pltpu.VMEM((2 * columns, half), f32),
    )
    held = pl.pallas_call(
        functools.partial(own_kernel, across, rows, len(ours)),
        out_shape=kept,
        in_specs=[vmem] * len(ours),
        out_specs=[vmem] * len(kept),
        cost_estimate=pl.CostEstimate(
            flops=2 * half * half * (width + LANES),
            transcendentals=half * half,
            bytes_accessed=2 * half * width,
        ),
    )(*in_vmem(ours))
    out = jax.ShapeDtypeStruct((columns, rows), f32)
    solution, residual = pl.pallas_call(
        functools.partial(solve_kernel, across, rows, len(theirs)),
        out_shape=(out, out),
        in_specs=[vmem] * (len(theirs) + len(kept)),
        out_specs=(vmem, vmem),
        scratch_shapes=[
            pltpu.VMEM((2 * half, width), bf16),
            pltpu.VMEM((2 * half, LANES), f32),
            pltpu.VMEM((8, 2 * half), f32),
            pltpu.VMEM((2 * half, 2 * half), bf16),
            pltpu.VMEM((2 * columns, 2 * half), bf16),
        ],
        cost_estimate=pl.CostEstimate(
            flops=6 * half * half * (width + LANES),
            transcendentals=3 * half * half,
            bytes_accessed=2 * half * width,
        ),
    )(*in_vmem(theirs), *in_vmem(held))
    return solution.T, residual.T


def fits_whole(sizes, points, targets):
    across, along, features = sizes
    rows, width = points.shape
    count = rows * across * along
    powers = all(size & (size - 1) == 0 for size in sizes)
    return (
        powers
        and along > 1
        and features == 2
        and 2 * rows == LANES
        and width == LANES
        and targets.shape[1] == 16
        and count % (2 * PANEL) == 0
        and 2 * count * count <= KERNEL_BYTES
        and ITERS == 2
    )


def local(sizes, points, targets):
    if fits_whole(sizes, points, targets):
        return whole_local(sizes, points, targets)
    return split_local(points, targets)


def solution(mesh):
    placed = (P(("gx", "gy"), "af"), P(("gx", "gy"), None))
    sizes = tuple(mesh.shape[axis] for axis in AXES)
    return jax.shard_map(
        functools.partial(local, sizes),
        mesh=mesh,
        in_specs=placed,
        out_specs=(P(("gx", "gy"), None), P(("gx", "gy"), None)),
        check_vma=False,
    )
```

```python
import functools
import math

import jax
import jax.numpy as jnp
from jax import lax
from jax.experimental import pallas as pl
from jax.experimental.pallas import tpu as pltpu
from jax.sharding import PartitionSpec as P


ITERS = 2


def point_norms(block):
    wide_block = block.astype(jnp.float32)
    return jnp.sum(wide_block * wide_block, axis=1)


def kernel_times(row_slab, slab_norms, col_slab, col_slab_norms, col_vector, scale):
    inner = lax.dot_general(
        row_slab, col_slab, (((1,), (1,)), ((), ())), preferred_element_type=jnp.float32
    )
    distance = slab_norms[:, None] + col_slab_norms[None, :] - 2.0 * inner
    kernel = jnp.exp(-scale * distance).astype(jnp.bfloat16)
    return jnp.dot(kernel, col_vector, preferred_element_type=jnp.float32)


def split_size(count):
    block_size = count
    while block_size > 1024 and block_size % 2 == 0:
        block_size = block_size // 2
    return block_size


def split_local(points, targets):
    whole_feat = lax.all_gather(points, "af", axis=1, tiled=True)
    norms = point_norms(whole_feat)
    half_rows = whole_feat.shape[0] // 2
    start_row = lax.axis_index("af") * half_rows
    my_points = lax.dynamic_slice_in_dim(whole_feat, start_row, half_rows, 0)
    scale = 0.5 / whole_feat.shape[1]
    stored_points = lax.all_gather(my_points, ("gx", "gy"), axis=0, tiled=True)
    stored_norms = point_norms(stored_points)

    def operate(vector):
        lowered = vector.astype(jnp.bfloat16)
        my_vector = lax.dynamic_slice_in_dim(lowered, start_row, half_rows, 0)
        empty = jnp.zeros(vector.shape, jnp.float32)
        piece = lax.all_gather(my_vector, ("gx", "gy"), axis=0, tiled=True)
        count = piece.shape[0]
        block_size = split_size(count)

        def one_block(carry, index):
            offset = index * block_size
            col_slab = lax.dynamic_slice_in_dim(stored_points, offset, block_size, 0)
            col_slab_norms = lax.dynamic_slice_in_dim(stored_norms, offset, block_size, 0)
            vector_slab = lax.dynamic_slice_in_dim(piece, offset, block_size, 0)
            return (
                carry
                + kernel_times(whole_feat, norms, col_slab, col_slab_norms, vector_slab, scale),
                None,
            )

        result, _ = lax.scan(one_block, empty, jnp.arange(count // block_size, dtype=jnp.int32))
        return lax.psum(result, "af") + 0.1 * vector

    def two_products(values, image):
        return lax.psum(
            (jnp.sum(values * values, axis=0), jnp.sum(values * image, axis=0)), ("gx", "gy")
        )

    solution = jnp.zeros_like(targets)
    residual = targets
    image = operate(residual)
    norm_now, product = two_products(residual, image)
    alpha = norm_now / product
    direction = residual
    along = image
    for step in range(ITERS):
        solution = solution + alpha * direction
        residual = residual - alpha * along
        if step + 1 < ITERS:
            image = operate(residual)
            norm_next, product = two_products(residual, image)
            ratio = norm_next / norm_now
            alpha = norm_next / (product - ratio * norm_next / alpha)
            direction = residual + ratio * direction
            along = image + ratio * along
            norm_now = norm_next
    return (solution, residual)


AXES = ("gx", "gy", "af")
LANES = 128
PANEL = 4 * LANES
EYE_COST = pl.CostEstimate(flops=20000000, transcendentals=0, bytes_accessed=65536)
KERNEL_BYTES = 8 * 1024 * 1024


def pack_kernel(points, turned, own, packed):
    wide = turned[...]
    high = wide.astype(jnp.bfloat16)
    low = (wide - high.astype(jnp.float32)).astype(jnp.bfloat16)
    both = jnp.concatenate([high, low], axis=1)
    packed[...] = both
    own[: points.shape[0], :] = points[...]
    own[points.shape[0] :, :] = both


def row_dot(a, b):
    return lax.dot_general(a, b, (((1,), (1,)), ((), ())), preferred_element_type=jnp.float32)


def plain_dot(a, b):
    return jnp.dot(a, b, preferred_element_type=jnp.float32)


def turn_of(features):
    return math.log2(math.e) * 0.5 / features


def unpack(blocks, rows, columns, groups, coords, parts):
    group = blocks * rows
    packed = []
    for index, (main, other) in enumerate(groups):
        width = main.shape[1]
        coords[index * group : (index + 1) * group, :width] = main[:group, :]
        coords[index * group : (index + 1) * group, width:] = other[...]
        for block in range(blocks):
            both = main[group + block * columns : group + (block + 1) * columns, :]
            packed.append(both.astype(jnp.float32))
    left = lax.broadcasted_iota(jnp.int32, packed[0].shape, 1) < rows
    for k in range(len(packed) // 2):
        one, two = packed[2 * k : 2 * k + 2]
        high = jnp.where(left, one, pltpu.roll(two, rows, 1))
        low = jnp.where(left, pltpu.roll(one, rows, 1), two)
        stacked = jnp.concatenate([high, low], axis=0).astype(jnp.bfloat16)
        parts[:, k * LANES : (k + 1) * LANES] = stacked


def eye_kernel(eye):
    rows = lax.broadcasted_iota(jnp.int32, eye.shape, 0)
    eye[...] = (rows == lax.broadcasted_iota(jnp.int32, eye.shape, 1)).astype(jnp.float32)


def scaled_norms(coords, start, down, along, eye):
    turn = turn_of(coords.shape[1])
    wide = coords[start : start + PANEL, :].astype(jnp.float32)
    column = -turn * jnp.sum(wide * wide, axis=1, keepdims=True)
    spread = jnp.broadcast_to(column, (PANEL, LANES))
    down[start : start + PANEL, :] = spread
    for k in range(PANEL // LANES):
        picked = eye[...] * spread[k * LANES : (k + 1) * LANES, :]
        row = jnp.sum(picked, axis=0, keepdims=True)
        first = start + k * LANES
        along[:, first : first + LANES] = jnp.broadcast_to(row, (8, LANES))


def kernel_columns(coords, down, along, kernel, begin, end, start):
    turn = turn_of(coords.shape[1])
    inner = row_dot(coords[begin:end, :], coords[start : start + PANEL, :])
    column = down[begin:end, :]
    column = jnp.concatenate([column] * (PANEL // LANES), axis=1)
    power = (2.0 * turn) * inner + column + along[:1, start : start + PANEL]
    kernel[begin:end, start : start + PANEL] = jnp.exp2(power).astype(jnp.bfloat16)


def join(parts):
    half = parts.shape[0] // 2
    return parts[:half, :] + parts[half:, :]


def own_kernel(blocks, rows, count, *refs):
    eye, coords, down, along, kernel, parts, image = refs[count:]
    groups = [(refs[k], refs[k + 1]) for k in range(0, count, 2)]
    unpack(blocks, rows, parts.shape[0] // 2, groups, coords, parts)
    half = coords.shape[0]
    for i in range(0, half, PANEL):
        scaled_norms(coords, i, down, along, eye)
    for j in range(0, half, PANEL):
        kernel_columns(coords, down, along, kernel, 0, half, j)
        image[:, j : j + PANEL] = plain_dot(parts[...], kernel[:, j : j + PANEL])


def solve_kernel(blocks, rows, count, *refs):
    eye, own, own_down, own_along, own_block, own_parts, own_image = refs[count : count + 7]
    solution_ref, residual_ref = refs[count + 7 : count + 9]
    coords, down, along, kernel, parts = refs[count + 9 :]
    groups = [(refs[k], refs[k + 1]) for k in range(0, count, 2)]
    half = own.shape[0]
    whole = 2 * half
    unpack(
        blocks, rows, parts.shape[0] // 2, groups, coords.at[half:, :], parts.at[:, half:]
    )
    coords[:half, :] = own[...]
    down[:half, :] = own_down[...]
    along[:, :half] = own_along[...]
    parts[:, :half] = own_parts[...]
    for i in range(half, whole, PANEL):
        scaled_norms(coords, i, down, along, eye)
    for j in range(0, half, PANEL):
        kernel_columns(coords, down, along, kernel, half, whole, j)
    for j in range(half, whole, PANEL):
        kernel_columns(coords, down, along, kernel, 0, whole, j)
    products = [
        own_image[...] + plain_dot(parts[:, half:], kernel[half:, :half]),
        plain_dot(parts[...], kernel[:, half:]),
    ]
    kernel[:half, :half] = own_block[...]
    targets = join(parts[...].astype(jnp.float32))

    def total_of(a, b):
        return jnp.sum(a * b, axis=1, keepdims=True)

    image = join(jnp.concatenate(products, axis=1)) + 0.1 * targets
    high = image.astype(jnp.bfloat16)
    low = (image - high.astype(jnp.float32)).astype(jnp.bfloat16)
    stacked = jnp.concatenate([high, low], axis=0)
    again = join(plain_dot(stacked, kernel[...])) + 0.1 * image
    norm_first = total_of(targets, targets)
    alpha = norm_first / total_of(targets, image)
    residual = targets - alpha * image
    norm_next = total_of(residual, residual)
    ratio = norm_next / norm_first
    direction = residual + ratio * targets
    along_direction = (1.0 + ratio) * image - alpha * again
    step = norm_next / total_of(direction, along_direction)
    solution_ref[...] = (alpha * targets + step * direction)[:, :rows]
    residual_ref[...] = (residual - step * along_direction)[:, :rows]


def swap(array, sizes, flips):
    pairs = []
    for place in range(math.prod(sizes)):
        rest, far, weight = place, 0, 1
        for size, flip in zip(reversed(sizes), reversed(flips)):
            far += ((rest % size) ^ flip) * weight
            rest, weight = rest // size, weight * size
        pairs.append((place, far))
    return lax.ppermute(array, AXES, pairs)


def in_vmem(arrays):
    return [pltpu.with_memory_space_constraint(array, pltpu.VMEM) for array in arrays]


def whole_local(sizes, points, targets):
    across, along, features = sizes
    rows = points.shape[0]
    columns = targets.shape[1]
    vmem = pl.BlockSpec(memory_space=pltpu.VMEM)
    eye = pl.pallas_call(
        eye_kernel,
        out_shape=pltpu.VMEM((LANES, LANES), jnp.float32),
        out_specs=vmem,
        cost_estimate=EYE_COST,
    )()
    early = across // 2
    early_points = swap(points, sizes, (early, 0, 0))
    packed_shape = (columns, 2 * rows)
    own, packed = pl.pallas_call(
        pack_kernel,
        out_shape=(
            pltpu.VMEM((rows + columns, LANES), jnp.bfloat16),
            pltpu.VMEM(packed_shape, jnp.bfloat16),
        ),
        in_specs=[vmem, vmem],
        out_specs=(vmem, vmem),
    )(*in_vmem([points, targets.T]))
    blocks = {0: own}
    for k in reversed(range(1, across)):
        if k != early:
            blocks[k] = swap(own, sizes, (k, 0, 0))
    late = swap(packed, sizes, (early, 0, 0))
    order = range(across)
    coords = [early_points if k == early else blocks[k][:rows] for k in order]
    coords = jnp.concatenate(coords, axis=0)
    parts = [late if k == early else blocks[k][rows:] for k in order]
    main = jnp.concatenate([coords, *parts], axis=0)
    moves = [(y, x) for y in range(0, along, 2) for x in range(features)]
    got = {}
    for y, x in reversed(moves):
        if (y, x) == (0, 0):
            got[y, x] = main
        else:
            got[y, x] = swap(coords if x else main, sizes, (0, y, x))
    ours = [got[move] for move in moves]
    theirs = [swap(block, sizes, (0, 1, 0)) for block in ours]
    half = rows * across * along // 2
    width = points.shape[1] * features
    f32, bf16 = jnp.float32, jnp.bfloat16
    vmem = pl.BlockSpec(memory_space=pltpu.VMEM)
    kept = (
        pltpu.VMEM((half, width), bf16),
        pltpu.VMEM((half, LANES), f32),
        pltpu.VMEM((8, half), f32),
        pltpu.VMEM((half, half), bf16),
        pltpu.VMEM((2 * columns, half), bf16),
        pltpu.VMEM((2 * columns, half), f32),
    )
    held = pl.pallas_call(
        functools.partial(own_kernel, across, rows, len(ours)),
        out_shape=kept,
        in_specs=[vmem] * (len(ours) + 1),
        out_specs=[vmem] * len(kept),
        cost_estimate=pl.CostEstimate(
            flops=2 * half * half * (width + LANES),
            transcendentals=half * half,
            bytes_accessed=2 * half * width,
        ),
    )(*in_vmem([*ours, eye]))
    out = jax.ShapeDtypeStruct((columns, rows), f32)
    solution, residual = pl.pallas_call(
        functools.partial(solve_kernel, across, rows, len(theirs)),
        out_shape=(out, out),
        in_specs=[vmem] * (len(theirs) + 1 + len(kept)),
        out_specs=(vmem, vmem),
        scratch_shapes=[
            pltpu.VMEM((2 * half, width), bf16),
            pltpu.VMEM((2 * half, LANES), f32),
            pltpu.VMEM((8, 2 * half), f32),
            pltpu.VMEM((2 * half, 2 * half), bf16),
            pltpu.VMEM((2 * columns, 2 * half), bf16),
        ],
        cost_estimate=pl.CostEstimate(
            flops=6 * half * half * (width + LANES),
            transcendentals=3 * half * half,
            bytes_accessed=2 * half * width,
        ),
    )(*in_vmem([*theirs, eye, *held]))
    return solution.T, residual.T


def fits_whole(sizes, points, targets):
    across, along, features = sizes
    rows, width = points.shape
    count = rows * across * along
    powers = all(size & (size - 1) == 0 for size in sizes)
    return (
        powers
        and along > 1
        and features == 2
        and 2 * rows == LANES
        and width == LANES
        and targets.shape[1] == 16
        and count % (2 * PANEL) == 0
        and 2 * count * count <= KERNEL_BYTES
        and ITERS == 2
    )


def local(sizes, points, targets):
    if fits_whole(sizes, points, targets):
        return whole_local(sizes, points, targets)
    return split_local(points, targets)


def solution(mesh):
    placed = (P(("gx", "gy"), "af"), P(("gx", "gy"), None))
    sizes = tuple(mesh.shape[axis] for axis in AXES)
    return jax.shard_map(
        functools.partial(local, sizes),
        mesh=mesh,
        in_specs=placed,
        out_specs=(P(("gx", "gy"), None), P(("gx", "gy"), None)),
        check_vma=False,
    )
```

```python
import functools
import math

import jax
import jax.numpy as jnp
from jax import lax
from jax.experimental import pallas as pl
from jax.experimental.pallas import tpu as pltpu
from jax.sharding import PartitionSpec as P


ITERS = 2


def point_norms(block):
    wide_block = block.astype(jnp.float32)
    return jnp.sum(wide_block * wide_block, axis=1)


def kernel_times(row_slab, slab_norms, col_slab, col_slab_norms, col_vector, scale):
    inner = lax.dot_general(
        row_slab, col_slab, (((1,), (1,)), ((), ())), preferred_element_type=jnp.float32
    )
    distance = slab_norms[:, None] + col_slab_norms[None, :] - 2.0 * inner
    kernel = jnp.exp(-scale * distance).astype(jnp.bfloat16)
    return jnp.dot(kernel, col_vector, preferred_element_type=jnp.float32)


def split_size(count):
    block_size = count
    while block_size > 1024 and block_size % 2 == 0:
        block_size = block_size // 2
    return block_size


def split_local(points, targets):
    whole_feat = lax.all_gather(points, "af", axis=1, tiled=True)
    norms = point_norms(whole_feat)
    half_rows = whole_feat.shape[0] // 2
    start_row = lax.axis_index("af") * half_rows
    my_points = lax.dynamic_slice_in_dim(whole_feat, start_row, half_rows, 0)
    scale = 0.5 / whole_feat.shape[1]
    stored_points = lax.all_gather(my_points, ("gx", "gy"), axis=0, tiled=True)
    stored_norms = point_norms(stored_points)

    def operate(vector):
        lowered = vector.astype(jnp.bfloat16)
        my_vector = lax.dynamic_slice_in_dim(lowered, start_row, half_rows, 0)
        empty = jnp.zeros(vector.shape, jnp.float32)
        piece = lax.all_gather(my_vector, ("gx", "gy"), axis=0, tiled=True)
        count = piece.shape[0]
        block_size = split_size(count)

        def one_block(carry, index):
            offset = index * block_size
            col_slab = lax.dynamic_slice_in_dim(stored_points, offset, block_size, 0)
            col_slab_norms = lax.dynamic_slice_in_dim(stored_norms, offset, block_size, 0)
            vector_slab = lax.dynamic_slice_in_dim(piece, offset, block_size, 0)
            return (
                carry
                + kernel_times(whole_feat, norms, col_slab, col_slab_norms, vector_slab, scale),
                None,
            )

        result, _ = lax.scan(one_block, empty, jnp.arange(count // block_size, dtype=jnp.int32))
        return lax.psum(result, "af") + 0.1 * vector

    def two_products(values, image):
        return lax.psum(
            (jnp.sum(values * values, axis=0), jnp.sum(values * image, axis=0)), ("gx", "gy")
        )

    solution = jnp.zeros_like(targets)
    residual = targets
    image = operate(residual)
    norm_now, product = two_products(residual, image)
    alpha = norm_now / product
    direction = residual
    along = image
    for step in range(ITERS):
        solution = solution + alpha * direction
        residual = residual - alpha * along
        if step + 1 < ITERS:
            image = operate(residual)
            norm_next, product = two_products(residual, image)
            ratio = norm_next / norm_now
            alpha = norm_next / (product - ratio * norm_next / alpha)
            direction = residual + ratio * direction
            along = image + ratio * along
            norm_now = norm_next
    return (solution, residual)


AXES = ("gx", "gy", "af")
LANES = 128
PANEL = 4 * LANES
EYE_COST = pl.CostEstimate(flops=20000000, transcendentals=0, bytes_accessed=65536)
KERNEL_BYTES = 8 * 1024 * 1024


def pack_kernel(points, turned, own, packed):
    wide = turned[...]
    high = wide.astype(jnp.bfloat16)
    low = (wide - high.astype(jnp.float32)).astype(jnp.bfloat16)
    both = jnp.concatenate([high, low], axis=1)
    packed[...] = both
    own[: points.shape[0], :] = points[...]
    own[points.shape[0] :, :] = both


def row_dot(a, b):
    return lax.dot_general(a, b, (((1,), (1,)), ((), ())), preferred_element_type=jnp.float32)


def plain_dot(a, b):
    return jnp.dot(a, b, preferred_element_type=jnp.float32)


def turn_of(features):
    return math.log2(math.e) * 0.5 / features


def unpack(blocks, rows, columns, groups, coords, parts):
    group = blocks * rows
    packed = []
    for index, (main, other) in enumerate(groups):
        width = main.shape[1]
        coords[index * group : (index + 1) * group, :width] = main[:group, :]
        coords[index * group : (index + 1) * group, width:] = other[...]
        for block in range(blocks):
            both = main[group + block * columns : group + (block + 1) * columns, :]
            packed.append(both.astype(jnp.float32))
    left = lax.broadcasted_iota(jnp.int32, packed[0].shape, 1) < rows
    for k in range(len(packed) // 2):
        one, two = packed[2 * k : 2 * k + 2]
        high = jnp.where(left, one, pltpu.roll(two, rows, 1))
        low = jnp.where(left, pltpu.roll(one, rows, 1), two)
        stacked = jnp.concatenate([high, low], axis=0).astype(jnp.bfloat16)
        parts[:, k * LANES : (k + 1) * LANES] = stacked


def eye_kernel(eye):
    rows = lax.broadcasted_iota(jnp.int32, eye.shape, 0)
    eye[...] = (rows == lax.broadcasted_iota(jnp.int32, eye.shape, 1)).astype(jnp.float32)


def scaled_norms(coords, start, down, along, eye):
    turn = turn_of(coords.shape[1])
    wide = coords[start : start + PANEL, :].astype(jnp.float32)
    column = -turn * jnp.sum(wide * wide, axis=1, keepdims=True)
    spread = jnp.broadcast_to(column, (PANEL, LANES))
    down[start : start + PANEL, :] = spread
    for k in range(PANEL // LANES):
        picked = eye[...] * spread[k * LANES : (k + 1) * LANES, :]
        row = jnp.sum(picked, axis=0, keepdims=True)
        first = start + k * LANES
        along[:, first : first + LANES] = jnp.broadcast_to(row, (8, LANES))


def kernel_columns(coords, down, along, kernel, begin, end, start, size=PANEL):
    turn = turn_of(coords.shape[1])
    inner = row_dot(coords[begin:end, :], coords[start : start + size, :])
    column = down[begin:end, :]
    column = jnp.concatenate([column] * (size // LANES), axis=1)
    power = (2.0 * turn) * inner + column + along[:1, start : start + size]
    kernel[begin:end, start : start + size] = jnp.exp2(power).astype(jnp.bfloat16)


def join(parts):
    half = parts.shape[0] // 2
    return parts[:half, :] + parts[half:, :]


def own_kernel(blocks, rows, count, *refs):
    eye, coords, down, along, kernel, parts, image = refs[count:]
    groups = [(refs[k], refs[k + 1]) for k in range(0, count, 2)]
    unpack(blocks, rows, parts.shape[0] // 2, groups, coords, parts)
    half = coords.shape[0]
    for i in range(0, half, PANEL):
        scaled_norms(coords, i, down, along, eye)
    for j in range(0, half, PANEL):
        kernel_columns(coords, down, along, kernel, 0, half, j)
        image[:, j : j + PANEL] = plain_dot(parts[...], kernel[:, j : j + PANEL])


def solve_kernel(blocks, rows, count, *refs):
    eye, own, own_down, own_along, own_block, own_parts, own_image = refs[count : count + 7]
    solution_ref, residual_ref = refs[count + 7 : count + 9]
    coords, down, along, kernel, parts = refs[count + 9 :]
    groups = [(refs[k], refs[k + 1]) for k in range(0, count, 2)]
    half = own.shape[0]
    whole = 2 * half
    unpack(
        blocks, rows, parts.shape[0] // 2, groups, coords.at[half:, :], parts.at[:, half:]
    )
    coords[:half, :] = own[...]
    down[:half, :] = own_down[...]
    along[:, :half] = own_along[...]
    parts[:, :half] = own_parts[...]
    for i in range(half, whole, PANEL):
        scaled_norms(coords, i, down, along, eye)
    kernel_columns(coords, down, along, kernel, half, whole, 0, whole)
    kernel_columns(coords, down, along, kernel, 0, half, half, half)
    products = [
        own_image[...] + plain_dot(parts[:, half:], kernel[half:, :half]),
        plain_dot(parts[...], kernel[:, half:]),
    ]
    kernel[:half, :half] = own_block[...]
    targets = join(parts[...].astype(jnp.float32))

    def total_of(a, b):
        return jnp.sum(a * b, axis=1, keepdims=True)

    image = join(jnp.concatenate(products, axis=1)) + 0.1 * targets
    high = image.astype(jnp.bfloat16)
    low = (image - high.astype(jnp.float32)).astype(jnp.bfloat16)
    stacked = jnp.concatenate([high, low], axis=0)
    again = join(plain_dot(stacked, kernel[...])) + 0.1 * image
    norm_first = total_of(targets, targets)
    alpha = norm_first / total_of(targets, image)
    residual = targets - alpha * image
    norm_next = total_of(residual, residual)
    ratio = norm_next / norm_first
    direction = residual + ratio * targets
    along_direction = (1.0 + ratio) * image - alpha * again
    step = norm_next / total_of(direction, along_direction)
    solution_ref[...] = (alpha * targets + step * direction)[:, :rows]
    residual_ref[...] = (residual - step * along_direction)[:, :rows]


def swap(array, sizes, flips):
    pairs = []
    for place in range(math.prod(sizes)):
        rest, far, weight = place, 0, 1
        for size, flip in zip(reversed(sizes), reversed(flips)):
            far += ((rest % size) ^ flip) * weight
            rest, weight = rest // size, weight * size
        pairs.append((place, far))
    return lax.ppermute(array, AXES, pairs)


def in_vmem(arrays):
    return [pltpu.with_memory_space_constraint(array, pltpu.VMEM) for array in arrays]


def whole_local(sizes, points, targets):
    across, along, features = sizes
    rows = points.shape[0]
    columns = targets.shape[1]
    vmem = pl.BlockSpec(memory_space=pltpu.VMEM)
    eye = pl.pallas_call(
        eye_kernel,
        out_shape=pltpu.VMEM((LANES, LANES), jnp.float32),
        out_specs=vmem,
        cost_estimate=EYE_COST,
    )()
    early = across // 2
    early_points = swap(points, sizes, (early, 0, 0))
    packed_shape = (columns, 2 * rows)
    own, packed = pl.pallas_call(
        pack_kernel,
        out_shape=(
            pltpu.VMEM((rows + columns, LANES), jnp.bfloat16),
            pltpu.VMEM(packed_shape, jnp.bfloat16),
        ),
        in_specs=[vmem, vmem],
        out_specs=(vmem, vmem),
    )(*in_vmem([points, targets.T]))
    blocks = {0: own}
    for k in reversed(range(1, across)):
        if k != early:
            blocks[k] = swap(own, sizes, (k, 0, 0))
    late = swap(packed, sizes, (early, 0, 0))
    order = range(across)
    coords = [early_points if k == early else blocks[k][:rows] for k in order]
    coords = jnp.concatenate(coords, axis=0)
    parts = [late if k == early else blocks[k][rows:] for k in order]
    main = jnp.concatenate([coords, *parts], axis=0)
    moves = [(y, x) for y in range(0, along, 2) for x in range(features)]
    got = {}
    for y, x in reversed(moves):
        if (y, x) == (0, 0):
            got[y, x] = main
        else:
            got[y, x] = swap(coords if x else main, sizes, (0, y, x))
    ours = [got[move] for move in moves]
    theirs = [swap(block, sizes, (0, 1, 0)) for block in ours]
    half = rows * across * along // 2
    width = points.shape[1] * features
    f32, bf16 = jnp.float32, jnp.bfloat16
    vmem = pl.BlockSpec(memory_space=pltpu.VMEM)
    kept = (
        pltpu.VMEM((half, width), bf16),
        pltpu.VMEM((half, LANES), f32),
        pltpu.VMEM((8, half), f32),
        pltpu.VMEM((half, half), bf16),
        pltpu.VMEM((2 * columns, half), bf16),
        pltpu.VMEM((2 * columns, half), f32),
    )
    held = pl.pallas_call(
        functools.partial(own_kernel, across, rows, len(ours)),
        out_shape=kept,
        in_specs=[vmem] * (len(ours) + 1),
        out_specs=[vmem] * len(kept),
        cost_estimate=pl.CostEstimate(
            flops=2 * half * half * (width + LANES),
            transcendentals=half * half,
            bytes_accessed=2 * half * width,
        ),
    )(*in_vmem([*ours, eye]))
    out = jax.ShapeDtypeStruct((columns, rows), f32)
    solution, residual = pl.pallas_call(
        functools.partial(solve_kernel, across, rows, len(theirs)),
        out_shape=(out, out),
        in_specs=[vmem] * (len(theirs) + 1 + len(kept)),
        out_specs=(vmem, vmem),
        scratch_shapes=[
            pltpu.VMEM((2 * half, width), bf16),
            pltpu.VMEM((2 * half, LANES), f32),
            pltpu.VMEM((8, 2 * half), f32),
            pltpu.VMEM((2 * half, 2 * half), bf16),
            pltpu.VMEM((2 * columns, 2 * half), bf16),
        ],
        cost_estimate=pl.CostEstimate(
            flops=6 * half * half * (width + LANES),
            transcendentals=3 * half * half,
            bytes_accessed=2 * half * width,
        ),
    )(*in_vmem([*theirs, eye, *held]))
    return solution.T, residual.T


def fits_whole(sizes, points, targets):
    across, along, features = sizes
    rows, width = points.shape
    count = rows * across * along
    powers = all(size & (size - 1) == 0 for size in sizes)
    return (
        powers
        and along > 1
        and features == 2
        and 2 * rows == LANES
        and width == LANES
        and targets.shape[1] == 16
        and count % (2 * PANEL) == 0
        and 2 * count * count <= KERNEL_BYTES
        and ITERS == 2
    )


def local(sizes, points, targets):
    if fits_whole(sizes, points, targets):
        return whole_local(sizes, points, targets)
    return split_local(points, targets)


def solution(mesh):
    placed = (P(("gx", "gy"), "af"), P(("gx", "gy"), None))
    sizes = tuple(mesh.shape[axis] for axis in AXES)
    return jax.shard_map(
        functools.partial(local, sizes),
        mesh=mesh,
        in_specs=placed,
        out_specs=(P(("gx", "gy"), None), P(("gx", "gy"), None)),
        check_vma=False,
    )
```

```python
import functools
import math

import jax
import jax.numpy as jnp
from jax import lax
from jax.experimental import pallas as pl
from jax.experimental.pallas import tpu as pltpu
from jax.sharding import PartitionSpec as P


ITERS = 2


def point_norms(block):
    wide_block = block.astype(jnp.float32)
    return jnp.sum(wide_block * wide_block, axis=1)


def kernel_times(row_slab, slab_norms, col_slab, col_slab_norms, col_vector, scale):
    inner = lax.dot_general(
        row_slab, col_slab, (((1,), (1,)), ((), ())), preferred_element_type=jnp.float32
    )
    distance = slab_norms[:, None] + col_slab_norms[None, :] - 2.0 * inner
    kernel = jnp.exp(-scale * distance).astype(jnp.bfloat16)
    return jnp.dot(kernel, col_vector, preferred_element_type=jnp.float32)


def split_size(count):
    block_size = count
    while block_size > 1024 and block_size % 2 == 0:
        block_size = block_size // 2
    return block_size


def split_local(points, targets):
    whole_feat = lax.all_gather(points, "af", axis=1, tiled=True)
    norms = point_norms(whole_feat)
    half_rows = whole_feat.shape[0] // 2
    start_row = lax.axis_index("af") * half_rows
    my_points = lax.dynamic_slice_in_dim(whole_feat, start_row, half_rows, 0)
    scale = 0.5 / whole_feat.shape[1]
    stored_points = lax.all_gather(my_points, ("gx", "gy"), axis=0, tiled=True)
    stored_norms = point_norms(stored_points)

    def operate(vector):
        lowered = vector.astype(jnp.bfloat16)
        my_vector = lax.dynamic_slice_in_dim(lowered, start_row, half_rows, 0)
        empty = jnp.zeros(vector.shape, jnp.float32)
        piece = lax.all_gather(my_vector, ("gx", "gy"), axis=0, tiled=True)
        count = piece.shape[0]
        block_size = split_size(count)

        def one_block(carry, index):
            offset = index * block_size
            col_slab = lax.dynamic_slice_in_dim(stored_points, offset, block_size, 0)
            col_slab_norms = lax.dynamic_slice_in_dim(stored_norms, offset, block_size, 0)
            vector_slab = lax.dynamic_slice_in_dim(piece, offset, block_size, 0)
            return (
                carry
                + kernel_times(whole_feat, norms, col_slab, col_slab_norms, vector_slab, scale),
                None,
            )

        result, _ = lax.scan(one_block, empty, jnp.arange(count // block_size, dtype=jnp.int32))
        return lax.psum(result, "af") + 0.1 * vector

    def two_products(values, image):
        return lax.psum(
            (jnp.sum(values * values, axis=0), jnp.sum(values * image, axis=0)), ("gx", "gy")
        )

    solution = jnp.zeros_like(targets)
    residual = targets
    image = operate(residual)
    norm_now, product = two_products(residual, image)
    alpha = norm_now / product
    direction = residual
    along = image
    for step in range(ITERS):
        solution = solution + alpha * direction
        residual = residual - alpha * along
        if step + 1 < ITERS:
            image = operate(residual)
            norm_next, product = two_products(residual, image)
            ratio = norm_next / norm_now
            alpha = norm_next / (product - ratio * norm_next / alpha)
            direction = residual + ratio * direction
            along = image + ratio * along
            norm_now = norm_next
    return (solution, residual)


AXES = ("gx", "gy", "af")
LANES = 128
PANEL = 2 * LANES
EYE_COST = pl.CostEstimate(flops=20000000, transcendentals=0, bytes_accessed=65536)
KERNEL_BYTES = 8 * 1024 * 1024


def pack_kernel(points, turned, own, packed):
    wide = turned[...]
    high = wide.astype(jnp.bfloat16)
    low = (wide - high.astype(jnp.float32)).astype(jnp.bfloat16)
    both = jnp.concatenate([high, low], axis=1)
    packed[...] = both
    own[: points.shape[0], :] = points[...]
    own[points.shape[0] :, :] = both


def row_dot(a, b):
    return lax.dot_general(a, b, (((1,), (1,)), ((), ())), preferred_element_type=jnp.float32)


def plain_dot(a, b):
    return jnp.dot(a, b, preferred_element_type=jnp.float32)


def turn_of(features):
    return math.log2(math.e) * 0.5 / features


def unpack(blocks, rows, columns, groups, coords, parts):
    group = blocks * rows
    packed = []
    for index, (main, other) in enumerate(groups):
        width = main.shape[1]
        coords[index * group : (index + 1) * group, :width] = main[:group, :]
        coords[index * group : (index + 1) * group, width:] = other[...]
        for block in range(blocks):
            both = main[group + block * columns : group + (block + 1) * columns, :]
            packed.append(both.astype(jnp.float32))
    left = lax.broadcasted_iota(jnp.int32, packed[0].shape, 1) < rows
    for k in range(len(packed) // 2):
        one, two = packed[2 * k : 2 * k + 2]
        high = jnp.where(left, one, pltpu.roll(two, rows, 1))
        low = jnp.where(left, pltpu.roll(one, rows, 1), two)
        stacked = jnp.concatenate([high, low], axis=0).astype(jnp.bfloat16)
        parts[:, k * LANES : (k + 1) * LANES] = stacked


def eye_kernel(eye):
    rows = lax.broadcasted_iota(jnp.int32, eye.shape, 0)
    eye[...] = (rows == lax.broadcasted_iota(jnp.int32, eye.shape, 1)).astype(jnp.float32)


def scaled_norms(coords, start, down, along, eye):
    turn = turn_of(coords.shape[1])
    wide = coords[start : start + PANEL, :].astype(jnp.float32)
    column = -turn * jnp.sum(wide * wide, axis=1, keepdims=True)
    spread = jnp.broadcast_to(column, (PANEL, LANES))
    down[start : start + PANEL, :] = spread
    for k in range(PANEL // LANES):
        picked = eye[...] * spread[k * LANES : (k + 1) * LANES, :]
        row = jnp.sum(picked, axis=0, keepdims=True)
        first = start + k * LANES
        along[:, first : first + LANES] = jnp.broadcast_to(row, (8, LANES))


def kernel_columns(coords, down, along, kernel, begin, end, start, size=PANEL):
    turn = turn_of(coords.shape[1])
    inner = row_dot(coords[begin:end, :], coords[start : start + size, :])
    column = down[begin:end, :]
    column = jnp.concatenate([column] * (size // LANES), axis=1)
    power = (2.0 * turn) * inner + column + along[:1, start : start + size]
    kernel[begin:end, start : start + size] = jnp.exp2(power).astype(jnp.bfloat16)


def join(parts):
    half = parts.shape[0] // 2
    return parts[:half, :] + parts[half:, :]


def own_kernel(blocks, rows, count, *refs):
    eye, coords, down, along, kernel, parts, image = refs[count:]
    groups = [(refs[k], refs[k + 1]) for k in range(0, count, 2)]
    unpack(blocks, rows, parts.shape[0] // 2, groups, coords, parts)
    half = coords.shape[0]
    for i in range(0, half, PANEL):
        scaled_norms(coords, i, down, along, eye)
    kernel_columns(coords, down, along, kernel, 0, half, 0, half)
    image[...] = plain_dot(parts[...], kernel[...])


def solve_kernel(blocks, rows, count, *refs):
    eye, own, own_down, own_along, own_block, own_parts, own_image = refs[count : count + 7]
    solution_ref, residual_ref = refs[count + 7 : count + 9]
    coords, down, along, kernel, parts = refs[count + 9 :]
    groups = [(refs[k], refs[k + 1]) for k in range(0, count, 2)]
    half = own.shape[0]
    whole = 2 * half
    unpack(
        blocks, rows, parts.shape[0] // 2, groups, coords.at[half:, :], parts.at[:, half:]
    )
    coords[:half, :] = own[...]
    down[:half, :] = own_down[...]
    along[:, :half] = own_along[...]
    parts[:, :half] = own_parts[...]
    for i in range(half, whole, PANEL):
        scaled_norms(coords, i, down, along, eye)
    kernel_columns(coords, down, along, kernel, half, whole, 0, whole)
    kernel_columns(coords, down, along, kernel, 0, half, half, half)
    products = [
        own_image[...] + plain_dot(parts[:, half:], kernel[half:, :half]),
        plain_dot(parts[...], kernel[:, half:]),
    ]
    kernel[:half, :half] = own_block[...]
    targets = join(parts[...].astype(jnp.float32))

    def total_of(a, b):
        return jnp.sum(a * b, axis=1, keepdims=True)

    image = join(jnp.concatenate(products, axis=1)) + 0.1 * targets
    high = image.astype(jnp.bfloat16)
    low = (image - high.astype(jnp.float32)).astype(jnp.bfloat16)
    stacked = jnp.concatenate([high, low], axis=0)
    again = join(plain_dot(stacked, kernel[...])) + 0.1 * image
    norm_first = total_of(targets, targets)
    alpha = norm_first / total_of(targets, image)
    residual = targets - alpha * image
    norm_next = total_of(residual, residual)
    ratio = norm_next / norm_first
    direction = residual + ratio * targets
    along_direction = (1.0 + ratio) * image - alpha * again
    step = norm_next / total_of(direction, along_direction)
    solution_ref[...] = (alpha * targets + step * direction)[:, :rows]
    residual_ref[...] = (residual - step * along_direction)[:, :rows]


def swap(array, sizes, flips):
    pairs = []
    for place in range(math.prod(sizes)):
        rest, far, weight = place, 0, 1
        for size, flip in zip(reversed(sizes), reversed(flips)):
            far += ((rest % size) ^ flip) * weight
            rest, weight = rest // size, weight * size
        pairs.append((place, far))
    return lax.ppermute(array, AXES, pairs)


def in_vmem(arrays):
    return [pltpu.with_memory_space_constraint(array, pltpu.VMEM) for array in arrays]


def whole_local(sizes, points, targets):
    across, along, features = sizes
    rows = points.shape[0]
    columns = targets.shape[1]
    vmem = pl.BlockSpec(memory_space=pltpu.VMEM)
    eye = pl.pallas_call(
        eye_kernel,
        out_shape=pltpu.VMEM((LANES, LANES), jnp.float32),
        out_specs=vmem,
        cost_estimate=EYE_COST,
    )()
    early = across // 2
    early_points = swap(points, sizes, (early, 0, 0))
    packed_shape = (columns, 2 * rows)
    own, packed = pl.pallas_call(
        pack_kernel,
        out_shape=(
            pltpu.VMEM((rows + columns, LANES), jnp.bfloat16),
            pltpu.VMEM(packed_shape, jnp.bfloat16),
        ),
        in_specs=[vmem, vmem],
        out_specs=(vmem, vmem),
    )(*in_vmem([points, targets.T]))
    blocks = {0: own}
    for k in reversed(range(1, across)):
        if k != early:
            blocks[k] = swap(own, sizes, (k, 0, 0))
    late = swap(packed, sizes, (early, 0, 0))
    order = range(across)
    coords = [early_points if k == early else blocks[k][:rows] for k in order]
    coords = jnp.concatenate(coords, axis=0)
    parts = [late if k == early else blocks[k][rows:] for k in order]
    main = jnp.concatenate([coords, *parts], axis=0)
    moves = [(y, x) for y in range(0, along, 2) for x in range(features)]
    got = {}
    for y, x in reversed(moves):
        if (y, x) == (0, 0):
            got[y, x] = main
        else:
            got[y, x] = swap(coords if x else main, sizes, (0, y, x))
    ours = [got[move] for move in moves]
    theirs = [swap(block, sizes, (0, 1, 0)) for block in ours]
    half = rows * across * along // 2
    width = points.shape[1] * features
    f32, bf16 = jnp.float32, jnp.bfloat16
    vmem = pl.BlockSpec(memory_space=pltpu.VMEM)
    kept = (
        pltpu.VMEM((half, width), bf16),
        pltpu.VMEM((half, LANES), f32),
        pltpu.VMEM((8, half), f32),
        pltpu.VMEM((half, half), bf16),
        pltpu.VMEM((2 * columns, half), bf16),
        pltpu.VMEM((2 * columns, half), f32),
    )
    held = pl.pallas_call(
        functools.partial(own_kernel, across, rows, len(ours)),
        out_shape=kept,
        in_specs=[vmem] * (len(ours) + 1),
        out_specs=[vmem] * len(kept),
        cost_estimate=pl.CostEstimate(
            flops=2 * half * half * (width + LANES),
            transcendentals=half * half,
            bytes_accessed=2 * half * width,
        ),
    )(*in_vmem([*ours, eye]))
    out = jax.ShapeDtypeStruct((columns, rows), f32)
    solution, residual = pl.pallas_call(
        functools.partial(solve_kernel, across, rows, len(theirs)),
        out_shape=(out, out),
        in_specs=[vmem] * (len(theirs) + 1 + len(kept)),
        out_specs=(vmem, vmem),
        scratch_shapes=[
            pltpu.VMEM((2 * half, width), bf16),
            pltpu.VMEM((2 * half, LANES), f32),
            pltpu.VMEM((8, 2 * half), f32),
            pltpu.VMEM((2 * half, 2 * half), bf16),
            pltpu.VMEM((2 * columns, 2 * half), bf16),
        ],
        cost_estimate=pl.CostEstimate(
            flops=6 * half * half * (width + LANES),
            transcendentals=3 * half * half,
            bytes_accessed=2 * half * width,
        ),
    )(*in_vmem([*theirs, eye, *held]))
    return solution.T, residual.T


def fits_whole(sizes, points, targets):
    across, along, features = sizes
    rows, width = points.shape
    count = rows * across * along
    powers = all(size & (size - 1) == 0 for size in sizes)
    return (
        powers
        and along > 1
        and features == 2
        and 2 * rows == LANES
        and width == LANES
        and targets.shape[1] == 16
        and count % (2 * PANEL) == 0
        and 2 * count * count <= KERNEL_BYTES
        and ITERS == 2
    )


def local(sizes, points, targets):
    if fits_whole(sizes, points, targets):
        return whole_local(sizes, points, targets)
    return split_local(points, targets)


def solution(mesh):
    placed = (P(("gx", "gy"), "af"), P(("gx", "gy"), None))
    sizes = tuple(mesh.shape[axis] for axis in AXES)
    return jax.shard_map(
        functools.partial(local, sizes),
        mesh=mesh,
        in_specs=placed,
        out_specs=(P(("gx", "gy"), None), P(("gx", "gy"), None)),
        check_vma=False,
    )
```
